32 devices in a mesh: seq: 4 (over x, core), ctx: 4 (over z), head: 2 (over y).
Axes of the slice: x: 2, y: 2, z: 4, core: 2. Of those that a mesh axis runs over, the one named last changes fastest.
Arguments:
- stream: bfloat16 [4, 256, 2880], P('seq', 'ctx'), may hold values from -6 to 6
- query_weight: bfloat16 [2880, 4096], P(None, 'head'), may hold values from -0.109375 to 0.109375
- cache_keys: bfloat16 [4, 8192, 8, 64], P('seq', 'ctx', 'head'), may hold values from -1000 to 1000
- cache_values: bfloat16 [4, 8192, 8, 64], P('seq', 'ctx', 'head'), may hold values from -6 to 6
- new_keys: bfloat16 [4, 256, 8, 64], P('seq', 'ctx', 'head'), may hold values from -18 to 18
- new_values: bfloat16 [4, 256, 8, 64], P('seq', 'ctx', 'head'), may hold values from -6 to 6
- out_weight: bfloat16 [4096, 2880], P('head'), may hold values from -0.09375 to 0.09375
- norm_gain: float32 [2880], replicated, may hold values from 0.5 to 1.5
- expert_ids: int32 [4, 256, 4], P('seq', 'ctx'), may hold values from 0 to 15, all different within a row; in each aligned block of 64 rows (0 to 63, 64 to 127, ..., all dimensions but the last counted through in order) at most 16 rows name the same one
- expert_weights: float32 [4, 256, 4], P('seq', 'ctx'), may hold values from 0.1 to 1
- gate_weight: bfloat16 [16, 2880, 2880], P(('seq', 'ctx'), None, 'head'), may hold values from -0.109375 to 0.109375
- up_weight: bfloat16 [16, 2880, 2880], P(('seq', 'ctx'), None, 'head'), may hold values from -0.109375 to 0.109375
- down_weight: bfloat16 [16, 2880, 2880], P(('seq', 'ctx'), 'head'), may hold values from -0.109375 to 0.109375
Outputs:
- mixed: bfloat16 [4, 256, 2880], P('seq', 'ctx', 'head')
The draws below stay inside these ranges and needn't reach their ends.
Inputs may be any that keep to these rules, and one draw needn't show every extreme that they name: `expert_ids`: in each aligned block of 64 rows (the tokens of one device) no expert is named by more than 16 rows; each row names 4 different experts.
All inputs are finite; a program needn't handle non-finite values.
Results may differ from the reference program's by a relative error of at most 0.015.
Values may be sent and summed in bfloat16 or wider, within the bound.
No kernel may reach another device: no remote copies, remote signals or barrier semaphores. Data moves between devices by JAX's collectives and lax.ppermute only.
A program may use at most 128 MiB of HBM per device.

```python
import math
import jax
import jax.numpy as jnp
import numpy as np
from jax import lax

D = 2880
HEADS = 64
KV_HEADS = 8
HEAD_DIM = 64
FF = 2880
TOPK = 4
Q_DEV = 64
EXPERTS = 16
BATCH = 4
NEW = 256
CACHE = 8192
CAP = 16
N_CTX = 4
N_HEAD = 2


def draw_cache_keys(key, part):
    shape = (BATCH, CACHE, KV_HEADS, HEAD_DIM)
    base = 2.5 * jax.random.truncated_normal(jax.random.fold_in(key, 11), -6.0, 6.0, shape, jnp.float32)
    return jnp.clip(base, -1000.0, 1000.0).astype(jnp.bfloat16)


def block_scale(rng, dims, cuts, low, top_value):
    factor_of, own = 1.0, jax.random.fold_in(rng, 6)
    for dim, blocks in cuts:
        draws = jnp.exp(jax.random.uniform(jax.random.fold_in(own, dim), (blocks,), jnp.float32, low / len(cuts), top_value / len(cuts)))
        factor_of = factor_of * jnp.repeat(draws, dims[dim] // blocks).reshape([-1 if axis == dim else 1 for axis in range(len(dims))])
    return factor_of


def shared_out(own_key, own, number, rows, count, top, most, skew):
    order = jax.random.permutation(own_key, count)
    crowded, common = portions_of(count, rows * top, most, skew, True), portions_of(count, rows * top, most, skew, False)
    places = jnp.arange(count)

    def named(lengths, turn):
        used = int((lengths > 0).sum())
        fixed = max(1, used // 4)
        shifted = fixed + (places - fixed + turn * (used - fixed)) % max(1, count - fixed)
        return jnp.zeros((count,), jnp.int32).at[order[jnp.where(places < fixed, places, shifted)]].set(jnp.asarray(lengths, jnp.int32))

    lengths = jnp.where(number % 4 == 0, named(crowded, number // 4), named(common, number - number // 4 - 1))
    mixed = jax.random.permutation(jax.random.fold_in(own, 3), count)
    giver, receiver = mixed[0:count // 2 * 2:2], mixed[1:count // 2 * 2:2]
    room = jnp.minimum(lengths[giver] - 1, most - lengths[receiver]) // 2
    room = jnp.where((giver == order[0]) | (receiver == order[0]) | (lengths[receiver] == 0), 0, jnp.maximum(room, 0))
    shifted = jax.random.randint(jax.random.fold_in(own, 4), (count // 2,), 0, 1 << 20) % (room + 1)
    lengths = lengths.at[giver].add(-shifted).at[receiver].add(shifted)
    items = jnp.searchsorted(jnp.cumsum(lengths), jnp.arange(rows * top), side="right").astype(jnp.int32)
    grid = items.reshape(top, rows).T
    grid = grid[jax.random.permutation(jax.random.fold_in(own, 1), rows)]
    turn = jax.random.randint(jax.random.fold_in(own, 2), (rows, 1), 0, top)
    return jnp.take_along_axis(grid, (jnp.arange(top)[None, :] + turn) % top, axis=1)


def portions_of(amount, total, reach, skew, full):
    portions = [(1 << 20) // math.isqrt(grade ** skew) + 1 for grade in range(1, amount + 1)]
    largest = reach if full else min(reach, max(-(-total // amount), total * portions[0] // sum(portions)))
    least = 1 if total - largest >= amount - 1 else 0
    given, spare = [largest] + [least] * (amount - 1), total - largest - least * (amount - 1)
    while spare > 0:
        movable = [i for i in range(1, amount) if given[i] < largest] or [i for i in range(1, amount) if given[i] < reach]
        pool, left = sum([portions[i] for i in movable]), spare
        for i in movable:
            addition = min(reach - given[i], max(1, left * portions[i] // pool), spare)
            given[i] = given[i] + addition
            spare = spare - addition
    return np.array(given)


def bell_draw(own_key, dims, deviation, reach, shards=(), held_as=jnp.bfloat16):
    level = block_scale(own_key, dims, shards, -0.22, 0.18) if shards else 1.0
    values = jax.random.normal(own_key, dims, jnp.float32) * deviation * level
    return jnp.minimum(jnp.maximum(values, -reach), reach).astype(held_as)


def setup_inputs(seed: int = 0) -> dict:
    splits = jax.random.split(jax.random.key(seed), 14)
    stream = bell_draw(splits[0], (BATCH, NEW, D), 1.0, 6.0, ((0, 4), (1, 4)))
    query_weight = bell_draw(splits[1], (D, HEADS * HEAD_DIM), D ** -0.5, 0.109375, ((1, 2),))
    cache_keys = draw_cache_keys(jax.random.fold_in(splits[13], 71), 0)
    cache_values = bell_draw(splits[3], (BATCH, CACHE, KV_HEADS, HEAD_DIM), 1.0, 6.0, ((0, 4), (1, 4), (2, 2)))
    new_keys = bell_draw(splits[4], (BATCH, NEW, KV_HEADS, HEAD_DIM), 3.0, 18.0, ((0, 4), (1, 4), (2, 2)))
    new_values = bell_draw(splits[5], (BATCH, NEW, KV_HEADS, HEAD_DIM), 1.0, 6.0, ((0, 4), (1, 4), (2, 2)))
    out_weight = bell_draw(splits[6], (HEADS * HEAD_DIM, D), (HEADS * HEAD_DIM) ** -0.5, 0.09375, ((0, 2),))
    norm_gain = jnp.clip(1.0 + 0.1 * jax.random.normal(splits[7], (D,), jnp.float32), 0.5, 1.5)
    expert_ids_keys = jax.random.split(jax.random.fold_in(splits[8], 1), BATCH * NEW // Q_DEV)
    expert_ids_turns = jax.random.permutation(jax.random.fold_in(splits[8], 3), BATCH * NEW // Q_DEV)
    expert_ids = jax.vmap(lambda own, number: shared_out(jax.random.fold_in(splits[8], 2), own, number, Q_DEV, EXPERTS, TOPK, CAP, 2))(expert_ids_keys, expert_ids_turns).reshape((BATCH, NEW, TOPK))
    expert_weights = jnp.clip(jnp.exp(math.log(1.0) - 2.3025851 * jax.random.uniform(splits[9], (BATCH, NEW, TOPK), jnp.float32) ** block_scale(splits[9], (BATCH, NEW, TOPK), ((0, 4), (1, 4)), -0.2, 0.2)), 0.1, 1.0)
    gate_weight = bell_draw(splits[10], (EXPERTS, D, FF), D ** -0.5, 0.109375, ((0, 16), (2, 2)))
    up_weight = bell_draw(splits[11], (EXPERTS, D, FF), D ** -0.5, 0.109375, ((0, 16), (2, 2)))
    down_weight = bell_draw(splits[12], (EXPERTS, FF, D), FF ** -0.5, 0.109375, ((0, 16), (1, 2)))
    return dict(stream=stream, query_weight=query_weight, cache_keys=cache_keys, cache_values=cache_values, new_keys=new_keys, new_values=new_values, out_weight=out_weight, norm_gain=norm_gain, expert_ids=expert_ids, expert_weights=expert_weights, gate_weight=gate_weight, up_weight=up_weight, down_weight=down_weight)


def attend_sequence(operands):
    query, keys, values = operands
    group = HEADS // KV_HEADS
    span = CACHE + NEW
    key_pos = lax.broadcasted_iota(jnp.int32, (NEW, span), 1)
    tok_pos = lax.broadcasted_iota(jnp.int32, (NEW, span), 0)
    allowed = (key_pos < CACHE) | (key_pos - CACHE <= tok_pos)
    grouped = query.reshape(NEW, KV_HEADS, group, HEAD_DIM).transpose(1, 0, 2, 3)
    keyed = keys.transpose(1, 0, 2)
    valued = values.transpose(1, 0, 2)

    def per_head(pieces):
        block, head_keys, head_values = pieces
        scores = jnp.einsum('tgd,jd->tgj', block.astype(jnp.float32), head_keys.astype(jnp.float32)) * (1.0 / math.sqrt(HEAD_DIM))
        scores = jnp.where(allowed[:, None, :], scores, -jnp.inf)
        top = lax.optimization_barrier(jnp.max(scores, axis=-1))
        weights = jnp.exp(scores - top[..., None])
        total = lax.optimization_barrier(jnp.sum(weights, axis=-1))
        probs = weights.astype(jnp.bfloat16)
        numerator = jnp.einsum('tgj,jd->tgd', probs.astype(jnp.float32), head_values.astype(jnp.float32))
        return (numerator / total[..., None]).astype(jnp.bfloat16)
    heads_out = lax.map(per_head, (grouped, keyed, valued))
    return heads_out.transpose(1, 0, 2, 3).reshape(NEW, HEADS * HEAD_DIM)

def reference(stream, query_weight, cache_keys, cache_values, new_keys, new_values, out_weight, norm_gain, expert_ids, expert_weights, gate_weight, up_weight, down_weight):
    tokens = stream.reshape(BATCH * NEW, D)
    query = jnp.dot(tokens, query_weight, preferred_element_type=jnp.float32).astype(jnp.bfloat16)
    query = query.reshape(BATCH, NEW, HEADS * HEAD_DIM)
    keys = jnp.concatenate([cache_keys, new_keys], axis=1)
    values = jnp.concatenate([cache_values, new_values], axis=1)
    attn = lax.map(attend_sequence, (query, keys, values)).reshape(BATCH * NEW, HEADS * HEAD_DIM)
    resid = tokens.astype(jnp.float32) + jnp.dot(attn, out_weight, preferred_element_type=jnp.float32)
    normed = (resid * lax.rsqrt(lax.optimization_barrier(jnp.mean(resid * resid, axis=-1, keepdims=True)) + 1e-05) * norm_gain).astype(jnp.bfloat16)
    blocks = BATCH * N_CTX
    pairs = Q_DEV * TOPK
    chosen = expert_ids.reshape(blocks, pairs)
    onehot = (chosen[:, :, None] == lax.broadcasted_iota(jnp.int32, (1, 1, EXPERTS), 2)).astype(jnp.int32)
    before = jnp.cumsum(onehot, axis=1) - onehot
    slot = lax.optimization_barrier(jnp.sum(before * onehot, axis=-1)).astype(jnp.int32)
    block_of = lax.broadcasted_iota(jnp.int32, (blocks, pairs), 0)
    pair_of = lax.broadcasted_iota(jnp.int32, (blocks, pairs), 1)
    row = (block_of * CAP + slot).reshape(-1).astype(jnp.int32)
    token_of = (block_of * Q_DEV + pair_of // TOPK).reshape(-1).astype(jnp.int32)
    flat_chosen = chosen.reshape(-1).astype(jnp.int32)
    buffer = jnp.zeros((EXPERTS, blocks * CAP, D), jnp.bfloat16).at[flat_chosen, row].set(normed[token_of])
    share = FF // N_HEAD

    def expert(operands):
        rows, gate_w, up_w, down_w = operands
        gate = jnp.dot(rows, gate_w, preferred_element_type=jnp.float32)
        up = jnp.dot(rows, up_w, preferred_element_type=jnp.float32)
        hidden = (gate * jax.nn.sigmoid(1.702 * gate) * (up + 1.0)).astype(jnp.bfloat16)
        parts = jnp.einsum('rgf,gfd->grd', hidden.reshape(rows.shape[0], N_HEAD, share).astype(jnp.float32), down_w.reshape(N_HEAD, share, D).astype(jnp.float32))
        parts = lax.optimization_barrier(parts.astype(jnp.bfloat16))
        return lax.optimization_barrier(jnp.sum(parts.astype(jnp.float32), axis=0)).astype(jnp.bfloat16)
    expert_out = lax.map(expert, (buffer, gate_weight, up_weight, down_weight))
    picked = expert_out[flat_chosen, row].astype(jnp.float32).reshape(BATCH * NEW, TOPK, D)
    moe = lax.optimization_barrier(jnp.sum(expert_weights.reshape(BATCH * NEW, TOPK, 1) * picked, axis=1))
    return (resid + moe).astype(jnp.bfloat16).reshape(BATCH, NEW, D)
```

```python
import math, functools
import jax, jax.numpy as jnp
from jax import lax
from jax.experimental import pallas as pl
from jax.experimental.pallas import tpu as pltpu
from jax.sharding import PartitionSpec as P


CAP = 16
TILE = 256
LANES = 128
NEG = -1e38


def attend_kernel(where_ref, q_ref, kk_ref, vv_ref, nk_ref, nv_ref, out_ref, s_ref, m_ref, *, tokens, kv, pairs, tile):
    half = LANES // 2
    rows = tokens * pairs * 2
    length = kk_ref.shape[2]
    tiles = length // tile
    factor = math.log2(math.e) / math.sqrt(half)
    place, source = where_ref[0], where_ref[1]

    def queries(h):
        lane = lax.broadcasted_iota(jnp.int32, (tokens, LANES), 1)
        pieces = []
        for p in range(pairs):
            start = pl.multiple_of((h * pairs + p) * LANES, LANES)
            block = q_ref[:, pl.ds(start, LANES)]
            pieces.append(jnp.where(lane < half, block, jnp.zeros_like(block)))
            pieces.append(jnp.where(lane < half, jnp.zeros_like(block), block))
        return jnp.concatenate(pieces, axis=0)

    def score_tile(h, slot, q, j, top):
        keys = kk_ref[h, :, j * tile:(j + 1) * tile]
        s = jnp.dot(q, jnp.concatenate([keys, keys], axis=0), preferred_element_type=jnp.float32)
        s_ref[slot, :, j * tile:(j + 1) * tile] = s
        for k in range(tile // LANES):
            part = s[:, k * LANES:(k + 1) * LANES]
            top = part if top is None else jnp.maximum(top, part)
        return top

    def score_new(h, slot, q, top):
        keys = nk_ref[h]
        s = jnp.dot(q, jnp.concatenate([keys, keys], axis=0), preferred_element_type=jnp.float32)
        col = lax.broadcasted_iota(jnp.int32, (rows, LANES), 1)
        tok = lax.broadcasted_iota(jnp.int32, (rows, LANES), 0) % tokens
        reach = jnp.where(place < source, tokens, jnp.where(place == source, 0, -tokens))
        s = jnp.where((col < tokens) & (col <= tok + reach), s, NEG)
        s_ref[slot, :, length:] = s
        top = jnp.maximum(top, s)
        m_ref[slot] = jnp.broadcast_to(jnp.max(top, axis=1, keepdims=True) * factor, (rows, LANES))

    def weigh(slot, start, width):
        m = m_ref[slot]
        out = []
        for k in range(width // LANES):
            out.append(jnp.exp2(s_ref[slot, :, start + k * LANES:start + (k + 1) * LANES] * factor - m).astype(jnp.bfloat16))
        return out[0] if len(out) == 1 else jnp.concatenate(out, axis=1)

    def value_tile(h, slot, j, acc):
        p = weigh(slot, j * tile, tile)
        o = gather_values(p, vv_ref[h, :, j * tile:(j + 1) * tile])
        return o if acc is None else acc + o

    def gather_values(p, values):
        values = jnp.concatenate([values, jnp.ones_like(values)], axis=0)
        return lax.dot_general(p, values, (((1,), (1,)), ((), ())), preferred_element_type=jnp.float32)

    def finish(h, slot, acc):
        acc = acc + gather_values(weigh(slot, length, LANES), nv_ref[h])
        lane = lax.broadcasted_iota(jnp.int32, (tokens, LANES), 1)
        low = lane < half
        stats = out_ref[:, kv * pairs * LANES:]
        for p in range(pairs):
            even = acc[2 * p * tokens:(2 * p + 1) * tokens]
            odd = acc[(2 * p + 1) * tokens:(2 * p + 2) * tokens]
            num = jnp.where(low, even, pltpu.roll(odd, half, 1))
            tot = jnp.where(low, pltpu.roll(even, half, 1), odd)
            m = jnp.where(low, m_ref[slot, 2 * p * tokens:(2 * p + 1) * tokens], m_ref[slot, (2 * p + 1) * tokens:(2 * p + 2) * tokens])
            index = h * pairs + p
            out_ref[:, pl.ds(pl.multiple_of(index * LANES, LANES), LANES)] = (num / tot).astype(jnp.bfloat16)
            lse = m + jnp.log2(tot)
            for piece in range(3):
                coarse = lse.astype(jnp.bfloat16)
                lse = lse - coarse.astype(jnp.float32)
                stats = jnp.where(lane % half == index + piece * kv * pairs, coarse, stats)
        out_ref[:, kv * pairs * LANES:] = stats

    out_ref[:, kv * pairs * LANES:] = jnp.zeros((tokens, LANES), jnp.bfloat16)
    q = queries(0)
    top = None
    for j in range(tiles):
        top = score_tile(0, 0, q, j, top)
    score_new(0, 0, q, top)

    def step(h, carry):
        slot = h % 2
        prev = 1 - slot
        q = queries(h)
        top = acc = None
        for j in range(tiles):
            top = score_tile(h, slot, q, j, top)
            acc = value_tile(h - 1, prev, j, acc)
        score_new(h, slot, q, top)
        finish(h - 1, prev, acc)
        return carry

    lax.fori_loop(1, kv, step, 0)
    acc = None
    last = (kv - 1) % 2
    for j in range(tiles):
        acc = value_tile(kv - 1, last, j, acc)
    finish(kv - 1, last, acc)


def attend(place, source, q, kk, vv, nk, nv, tile=TILE):
    tokens, width = q.shape
    kv, _, length = kk.shape
    pairs = width // LANES // kv
    rows = tokens * pairs * 2
    where = jnp.stack([place, source]).astype(jnp.int32)
    vm = pl.BlockSpec(memory_space=pltpu.VMEM)
    flops = 4 * rows * kv * (length + LANES) * LANES
    return pl.pallas_call(
        functools.partial(attend_kernel, tokens=tokens, kv=kv, pairs=pairs, tile=tile),
        out_shape=jax.ShapeDtypeStruct((tokens, width + LANES), jnp.bfloat16),
        in_specs=[pl.BlockSpec(memory_space=pltpu.SMEM)] + [vm] * 5,
        out_specs=vm,
        scratch_shapes=[pltpu.VMEM((2, rows, length + LANES), jnp.float32), pltpu.VMEM((2, rows, LANES), jnp.float32)],
        compiler_params=pltpu.CompilerParams(vmem_limit_bytes=32 * 1024 * 1024),
        cost_estimate=pl.CostEstimate(flops=flops * 2, bytes_accessed=0, transcendentals=0),
        name="attend",
    )(where, q, kk, vv, nk, nv)


def merge_kernel(*refs, count, group):
    packets, weight_ref, out_ref, attn_ref = refs[:count], refs[count], refs[count + 1], refs[count + 2]
    tokens = packets[0].shape[0]
    width = packets[0].shape[1] - LANES

    @pl.when(pl.program_id(0) == 0)
    def _():
        logs = []
        for packet in packets:
            pieces = packet[:, width:].astype(jnp.float32)
            logs.append(pieces + (pltpu.roll(pieces, LANES - group, 1) + pltpu.roll(pieces, LANES - 2 * group, 1)))
        top = functools.reduce(jnp.maximum, logs)
        shares = [jnp.exp2(log - top) for log in logs]
        total = functools.reduce(jnp.add, shares)
        split = []
        for share in shares:
            share = share / total
            coarse = share.astype(jnp.bfloat16)
            split.append(jnp.concatenate([coarse, (share - coarse.astype(jnp.float32)).astype(jnp.bfloat16)], axis=1))
        split = jnp.concatenate(split, axis=0)
        half = LANES // 2
        lanes = 2 * LANES
        row = lax.broadcasted_iota(jnp.int32, (lanes, lanes), 0) % LANES
        col = lax.broadcasted_iota(jnp.int32, (lanes, lanes), 1)
        for start in range(0, width, lanes):
            head = (col + start) // LANES + col % LANES // half * half
            spread = jnp.where(row == head, 1.0, 0.0).astype(jnp.bfloat16)
            wide = jnp.dot(split, spread, preferred_element_type=jnp.float32)
            attn = 0.0
            for i, packet in enumerate(packets):
                attn = attn + wide[i * tokens:(i + 1) * tokens] * packet[:, start:start + lanes].astype(jnp.float32)
            attn_ref[:, start:start + lanes] = attn.astype(jnp.bfloat16)

    part = lax.dot_general(weight_ref[...], attn_ref[...], TURNED, preferred_element_type=jnp.float32)
    out_ref[...] = part.T.astype(out_ref.dtype)


def merge_project(packets, weight, group, block=5 * LANES):
    tokens = packets[0].shape[0]
    model, depth = weight.shape
    vm = pl.BlockSpec(memory_space=pltpu.VMEM)
    return pl.pallas_call(
        functools.partial(merge_kernel, count=len(packets), group=group),
        out_shape=jax.ShapeDtypeStruct((tokens, model), jnp.bfloat16),
        grid=(pl.cdiv(model, block),),
        in_specs=[vm] * len(packets) + [pl.BlockSpec((block, depth), lambda k: (k, 0))],
        out_specs=pl.BlockSpec((tokens, block), lambda k: (0, k)),
        scratch_shapes=[pltpu.VMEM((tokens, depth), jnp.bfloat16)],
        compiler_params=pltpu.CompilerParams(vmem_limit_bytes=58 * 1024 * 1024),
        cost_estimate=pl.CostEstimate(flops=2 * tokens * depth * model, bytes_accessed=2 * depth * model, transcendentals=0),
        name="merge_project",
    )(*packets, weight)


def steps_of(extent, step):
    return [(start, min(start + step, extent)) for start in range(0, extent, step)]


TURNED = (((1,), (1,)), ((), ()))


def expert_kernel(rows_ref, gate_hbm, up_hbm, down_hbm, out_ref, gate_ref, up_ref, down_ref, act_ref, acc_ref, sems, *, step):
    hidden, model = gate_hbm.shape
    pairs = []
    for start, stop in steps_of(hidden, step):
        pairs.append((gate_hbm.at[start:stop], gate_ref.at[start:stop]))
        pairs.append((up_hbm.at[start:stop], up_ref.at[start:stop]))
    later = len(pairs)
    for start, stop in steps_of(hidden, step):
        pairs.append((down_hbm.at[start:stop], down_ref.at[start:stop]))
    copies = [pltpu.make_async_copy(source, target, sems.at[i]) for i, (source, target) in enumerate(pairs)]
    for copy in copies:
        copy.start()
    rows = rows_ref[...]
    for i, (start, stop) in enumerate(steps_of(hidden, step)):
        copies[2 * i].wait()
        copies[2 * i + 1].wait()
        gate = lax.dot_general(gate_ref[start:stop], rows, TURNED, preferred_element_type=jnp.float32)
        up = lax.dot_general(up_ref[start:stop], rows, TURNED, preferred_element_type=jnp.float32)
        act = gate * jax.nn.sigmoid(1.702 * gate) * (up + 1.0)
        act_ref[:, start:stop] = act.T.astype(jnp.bfloat16)
    for copy in copies[later:]:
        copy.wait()
    act = act_ref[...]
    for start, stop in steps_of(model, 4 * LANES):
        acc_ref[:, start:stop] = jnp.dot(act, down_ref[:, start:stop], preferred_element_type=jnp.float32)
    width = out_ref.shape[2]
    for i in range(out_ref.shape[0]):
        out_ref[i] = acc_ref[:, i * width:(i + 1) * width].astype(out_ref.dtype)


def expert(rows, gate, up, down, pieces, step=2 * LANES):
    count, model = rows.shape
    hidden = gate.shape[0]
    vm = pl.BlockSpec(memory_space=pltpu.VMEM)
    stay = pl.BlockSpec(memory_space=pl.ANY)
    return pl.pallas_call(
        functools.partial(expert_kernel, step=step),
        out_shape=jax.ShapeDtypeStruct((pieces, count, model // pieces), jnp.bfloat16),
        in_specs=[vm] + [stay] * 3,
        out_specs=vm,
        scratch_shapes=[
            pltpu.VMEM((hidden, model), jnp.bfloat16),
            pltpu.VMEM((hidden, model), jnp.bfloat16),
            pltpu.VMEM((hidden, model), jnp.bfloat16),
            pltpu.VMEM((count, hidden), jnp.bfloat16),
            pltpu.VMEM((count, model), jnp.float32),
            pltpu.SemaphoreType.DMA((3 * pl.cdiv(hidden, step),)),
        ],
        compiler_params=pltpu.CompilerParams(vmem_limit_bytes=56 * 1024 * 1024),
        cost_estimate=pl.CostEstimate(flops=6 * count * model * hidden, bytes_accessed=6 * model * hidden, transcendentals=0),
        name="expert",
    )(rows, gate, up, down)


def project_kernel(x_ref, weight_ref, out_ref):
    out_ref[...] = jnp.dot(x_ref[...], weight_ref[...], preferred_element_type=jnp.float32).astype(out_ref.dtype)


def project(x, weight, block=2 * LANES):
    tokens, model = x.shape
    width = weight.shape[1]
    return pl.pallas_call(
        project_kernel,
        out_shape=jax.ShapeDtypeStruct((tokens, width), jnp.bfloat16),
        grid=(pl.cdiv(width, block),),
        in_specs=[pl.BlockSpec((tokens, model), lambda n: (0, 0)), pl.BlockSpec((model, block), lambda n: (0, n))],
        out_specs=pl.BlockSpec((tokens, block), lambda n: (0, n)),
        compiler_params=pltpu.CompilerParams(vmem_limit_bytes=58 * 1024 * 1024),
        cost_estimate=pl.CostEstimate(flops=2 * tokens * model * width, bytes_accessed=2 * model * width, transcendentals=0),
        name="project",
    )(x, weight)


def shifted(block, axis, distance):
    size = lax.axis_size(axis)
    return lax.ppermute(block, axis, [(i, (i + distance) % size) for i in range(size)])


def body(
    stream,
    query_weight,
    cache_keys,
    cache_values,
    new_keys,
    new_values,
    out_weight,
    norm_gain,
    expert_ids,
    expert_weights,
    gate_weight,
    up_weight,
    down_weight,
):
    tokens = stream[0]
    count, model = tokens.shape
    cycles = lax.axis_size("ctx")
    heads = lax.axis_size("head")
    place = lax.axis_index("ctx")
    query = project(tokens, query_weight)

    def columns(x):
        return x[0].transpose(1, 2, 0)

    def padded(x):
        return jnp.pad(x, ((0, 0), (0, 0), (0, LANES - x.shape[2])))

    keys, values = columns(cache_keys), columns(cache_values)
    fresh_keys, fresh_values = padded(columns(new_keys)), padded(columns(new_values))
    packets = []
    block = query
    for d in range(cycles):
        following = shifted(block, "ctx", 1) if d < cycles - 1 else None
        packet = attend(place, (place - d) % cycles, block, keys, values, fresh_keys, fresh_values)
        if d < cycles - 1:
            following, packet = lax.optimization_barrier((following, packet))
        packets.append(packet if d == 0 else shifted(packet, "ctx", -d))
        block = following
    group = query.shape[1] // LANES
    projected = merge_project(packets, out_weight.T, group)
    resid = tokens.astype(jnp.float32) + projected.astype(jnp.float32)
    for d in range(1, heads):
        resid = resid + shifted(projected, "head", d).astype(jnp.float32)
    width = model // heads
    resid_own = lax.dynamic_slice_in_dim(resid, lax.axis_index("head") * width, width, 1)
    normed = (
        resid * lax.rsqrt(jnp.mean(resid * resid, axis=-1, keepdims=True) + 1e-05) * norm_gain
    ).astype(jnp.bfloat16)
    experts = lax.axis_size("seq") * lax.axis_size("ctx")
    slots = experts * CAP
    chosen = expert_ids[0].reshape(-1)
    onehot = (chosen[:, None] == lax.broadcasted_iota(jnp.int32, (1, experts), 1)).astype(jnp.int32)
    before = jnp.cumsum(onehot, axis=0) - onehot
    target = chosen * CAP + jnp.sum(before * onehot, axis=1)
    matches = target[None, :] == lax.broadcasted_iota(jnp.int32, (slots, 1), 0)
    select = jnp.sum(matches.astype(jnp.float32).reshape(slots, count, -1), axis=-1).astype(jnp.bfloat16)
    packed = jnp.dot(select, normed, preferred_element_type=jnp.float32).astype(jnp.bfloat16)
    packed = packed.reshape(experts, CAP, model)
    arrived = lax.all_to_all(packed, ("seq", "ctx"), split_axis=0, concat_axis=0, tiled=True)
    parts = expert(arrived.reshape(slots, model), gate_weight[0].T, up_weight[0].T, down_weight[0], heads)
    parts = parts.reshape(heads * experts, CAP, width)
    returned = lax.all_to_all(parts, ("head", "seq", "ctx"), split_axis=0, concat_axis=0, tiled=True)
    spread = jnp.where(matches.T, expert_weights[0].reshape(-1)[:, None], 0.0)
    spread = jnp.sum(spread.reshape(count, -1, slots), axis=1)
    moe = lax.dot_general(
        jnp.tile(spread, (1, heads)),
        returned.reshape(heads * slots, width).astype(jnp.float32),
        (((1,), (0,)), ((), ())),
        precision=lax.Precision.HIGHEST,
    )
    return (resid_own + moe).astype(jnp.bfloat16)[None]


def solution(mesh):
    in_specs = (
        P("seq", "ctx", None),
        P(None, "head"),
        P("seq", "ctx", "head", None),
        P("seq", "ctx", "head", None),
        P("seq", "ctx", "head", None),
        P("seq", "ctx", "head", None),
        P("head", None),
        P(),
        P("seq", "ctx", None),
        P("seq", "ctx", None),
        P(("seq", "ctx"), None, "head"),
        P(("seq", "ctx"), None, "head"),
        P(("seq", "ctx"), "head", None),
    )
    out_specs = P("seq", "ctx", "head")
    return jax.shard_map(body, mesh=mesh, in_specs=in_specs, out_specs=out_specs, check_vma=False)
```

```python
import math, functools
import jax, jax.numpy as jnp
from jax import lax
from jax.experimental import pallas as pl
from jax.experimental.pallas import tpu as pltpu
from jax.sharding import PartitionSpec as P


CAP = 16
TILE = 256
LANES = 128
NEG = -1e38


def attend_kernel(where_ref, q_ref, kk_ref, vv_ref, nk_ref, nv_ref, out_ref, s_ref, m_ref, *, tokens, kv, pairs, tile):
    half = LANES // 2
    rows = tokens * pairs * 2
    length = kk_ref.shape[2]
    tiles = length // tile
    factor = math.log2(math.e) / math.sqrt(half)
    place, source = where_ref[0], where_ref[1]

    def queries(h):
        lane = lax.broadcasted_iota(jnp.int32, (tokens, LANES), 1)
        pieces = []
        for p in range(pairs):
            start = pl.multiple_of((h * pairs + p) * LANES, LANES)
            block = q_ref[:, pl.ds(start, LANES)]
            pieces.append(jnp.where(lane < half, block, jnp.zeros_like(block)))
            pieces.append(jnp.where(lane < half, jnp.zeros_like(block), block))
        return jnp.concatenate(pieces, axis=0)

    def score_tile(h, slot, q, j, top):
        keys = kk_ref[h, :, j * tile:(j + 1) * tile]
        s = jnp.dot(q, jnp.concatenate([keys, keys], axis=0), preferred_element_type=jnp.float32)
        s_ref[slot, :, j * tile:(j + 1) * tile] = s
        for k in range(tile // LANES):
            part = s[:, k * LANES:(k + 1) * LANES]
            top = part if top is None else jnp.maximum(top, part)
        return top

    def score_new(h, slot, q, top):
        keys = nk_ref[h]
        s = jnp.dot(q, jnp.concatenate([keys, keys], axis=0), preferred_element_type=jnp.float32)
        col = lax.broadcasted_iota(jnp.int32, (rows, LANES), 1)
        tok = lax.broadcasted_iota(jnp.int32, (rows, LANES), 0) % tokens
        reach = jnp.where(place < source, tokens, jnp.where(place == source, 0, -tokens))
        s = jnp.where((col < tokens) & (col <= tok + reach), s, NEG)
        s_ref[slot, :, length:] = s
        top = jnp.maximum(top, s)
        m_ref[slot] = jnp.broadcast_to(jnp.max(top, axis=1, keepdims=True) * factor, (rows, LANES))

    def weigh(slot, start, width):
        m = m_ref[slot]
        out = []
        for k in range(width // LANES):
            out.append(jnp.exp2(s_ref[slot, :, start + k * LANES:start + (k + 1) * LANES] * factor - m).astype(jnp.bfloat16))
        return out[0] if len(out) == 1 else jnp.concatenate(out, axis=1)

    def value_tile(h, slot, j, acc):
        p = weigh(slot, j * tile, tile)
        o = gather_values(p, vv_ref[h, :, j * tile:(j + 1) * tile])
        return o if acc is None else acc + o

    def gather_values(p, values):
        values = jnp.concatenate([values, jnp.ones_like(values)], axis=0)
        return lax.dot_general(p, values, (((1,), (1,)), ((), ())), preferred_element_type=jnp.float32)

    def finish(h, slot, acc):
        acc = acc + gather_values(weigh(slot, length, LANES), nv_ref[h])
        lane = lax.broadcasted_iota(jnp.int32, (tokens, LANES), 1)
        low = lane < half
        stats = out_ref[:, kv * pairs * LANES:]
        for p in range(pairs):
            even = acc[2 * p * tokens:(2 * p + 1) * tokens]
            odd = acc[(2 * p + 1) * tokens:(2 * p + 2) * tokens]
            num = jnp.where(low, even, pltpu.roll(odd, half, 1))
            tot = jnp.where(low, pltpu.roll(even, half, 1), odd)
            m = jnp.where(low, m_ref[slot, 2 * p * tokens:(2 * p + 1) * tokens], m_ref[slot, (2 * p + 1) * tokens:(2 * p + 2) * tokens])
            index = h * pairs + p
            out_ref[:, pl.ds(pl.multiple_of(index * LANES, LANES), LANES)] = (num / tot).astype(jnp.bfloat16)
            lse = m + jnp.log2(tot)
            for piece in range(3):
                coarse = lse.astype(jnp.bfloat16)
                lse = lse - coarse.astype(jnp.float32)
                stats = jnp.where(lane % half == index + piece * kv * pairs, coarse, stats)
        out_ref[:, kv * pairs * LANES:] = stats

    out_ref[:, kv * pairs * LANES:] = jnp.zeros((tokens, LANES), jnp.bfloat16)
    q = queries(0)
    top = None
    for j in range(tiles):
        top = score_tile(0, 0, q, j, top)
    score_new(0, 0, q, top)

    def step(h, carry):
        slot = h % 2
        prev = 1 - slot
        q = queries(h)
        top = acc = None
        for j in range(tiles):
            top = score_tile(h, slot, q, j, top)
            acc = value_tile(h - 1, prev, j, acc)
        score_new(h, slot, q, top)
        finish(h - 1, prev, acc)
        return carry

    lax.fori_loop(1, kv, step, 0)
    acc = None
    last = (kv - 1) % 2
    for j in range(tiles):
        acc = value_tile(kv - 1, last, j, acc)
    finish(kv - 1, last, acc)


def attend(place, source, q, kk, vv, nk, nv, tile=TILE):
    tokens, width = q.shape
    kv, _, length = kk.shape
    pairs = width // LANES // kv
    rows = tokens * pairs * 2
    where = jnp.stack([place, source]).astype(jnp.int32)
    vm = pl.BlockSpec(memory_space=pltpu.VMEM)
    flops = 4 * rows * kv * (length + LANES) * LANES
    return pl.pallas_call(
        functools.partial(attend_kernel, tokens=tokens, kv=kv, pairs=pairs, tile=tile),
        out_shape=jax.ShapeDtypeStruct((tokens, width + LANES), jnp.bfloat16),
        in_specs=[pl.BlockSpec(memory_space=pltpu.SMEM)] + [vm] * 5,
        out_specs=vm,
        scratch_shapes=[pltpu.VMEM((2, rows, length + LANES), jnp.float32), pltpu.VMEM((2, rows, LANES), jnp.float32)],
        compiler_params=pltpu.CompilerParams(vmem_limit_bytes=32 * 1024 * 1024),
        cost_estimate=pl.CostEstimate(flops=flops * 2, bytes_accessed=0, transcendentals=0),
        name="attend",
    )(where, q, kk, vv, nk, nv)


def merge_kernel(*refs, count, group):
    packets, weight_ref, out_ref, attn_ref = refs[:count], refs[count], refs[count + 1], refs[count + 2]
    tokens = packets[0].shape[0]
    width = packets[0].shape[1] - LANES

    logs = []
    for packet in packets:
        pieces = packet[:, width:].astype(jnp.float32)
        logs.append(pieces + (pltpu.roll(pieces, LANES - group, 1) + pltpu.roll(pieces, LANES - 2 * group, 1)))
    top = functools.reduce(jnp.maximum, logs)
    shares = [jnp.exp2(log - top) for log in logs]
    total = functools.reduce(jnp.add, shares)
    split = []
    for share in shares:
        share = share / total
        coarse = share.astype(jnp.bfloat16)
        split.append(jnp.concatenate([coarse, (share - coarse.astype(jnp.float32)).astype(jnp.bfloat16)], axis=1))
    split = jnp.concatenate(split, axis=0)
    half = LANES // 2
    lanes = 2 * LANES
    row = lax.broadcasted_iota(jnp.int32, (lanes, lanes), 0) % LANES
    col = lax.broadcasted_iota(jnp.int32, (lanes, lanes), 1)
    for start in range(0, width, lanes):
        head = (col + start) // LANES + col % LANES // half * half
        spread = jnp.where(row == head, 1.0, 0.0).astype(jnp.bfloat16)
        wide = jnp.dot(split, spread, preferred_element_type=jnp.float32)
        attn = 0.0
        for i, packet in enumerate(packets):
            attn = attn + wide[i * tokens:(i + 1) * tokens] * packet[:, start:start + lanes].astype(jnp.float32)
        attn_ref[:, start:start + lanes] = attn.astype(jnp.bfloat16)

    for start, stop in steps_of(weight_ref.shape[0], 5 * LANES):
        part = lax.dot_general(weight_ref[start:stop], attn_ref[...], TURNED, preferred_element_type=jnp.float32)
        out_ref[:, start:stop] = part.T.astype(out_ref.dtype)


def merge_project(packets, weight, group):
    tokens = packets[0].shape[0]
    model, depth = weight.shape
    vm = pl.BlockSpec(memory_space=pltpu.VMEM)
    return pl.pallas_call(
        functools.partial(merge_kernel, count=len(packets), group=group),
        out_shape=jax.ShapeDtypeStruct((tokens, model), jnp.bfloat16),
        in_specs=[vm] * (len(packets) + 1),
        out_specs=vm,
        scratch_shapes=[pltpu.VMEM((tokens, depth), jnp.bfloat16)],
        compiler_params=pltpu.CompilerParams(vmem_limit_bytes=12 * 1024 * 1024),
        cost_estimate=pl.CostEstimate(flops=2 * tokens * depth * model, bytes_accessed=2 * depth * model, transcendentals=0),
        name="merge_project",
    )(*packets, weight)


def steps_of(extent, step):
    return [(start, min(start + step, extent)) for start in range(0, extent, step)]


TURNED = (((1,), (1,)), ((), ()))


def fetch_kernel(*refs, count, step):
    sources, targets, sems = refs[:count], refs[count + 1:2 * count + 1], refs[2 * count + 1]
    pairs = []
    for source, target in zip(sources, targets):
        for start, stop in steps_of(source.shape[0], step):
            pairs.append((source.at[start:stop], target.at[start:stop]))
    copies = [pltpu.make_async_copy(source, target, sems.at[i]) for i, (source, target) in enumerate(pairs)]
    for copy in copies:
        copy.start()
    for copy in copies:
        copy.wait()


def fetch(arrays, after, step=3 * LANES):
    stay = pl.BlockSpec(memory_space=pl.ANY)
    number = sum(pl.cdiv(array.shape[0], step) for array in arrays)
    size = sum(2 * array.size for array in arrays)
    return pl.pallas_call(
        functools.partial(fetch_kernel, count=len(arrays), step=step),
        out_shape=[pltpu.VMEM(array.shape, array.dtype) for array in arrays],
        in_specs=[stay] * (len(arrays) + 1),
        out_specs=[pl.BlockSpec(memory_space=pltpu.VMEM)] * len(arrays),
        scratch_shapes=[pltpu.SemaphoreType.DMA((number,))],
        compiler_params=pltpu.CompilerParams(vmem_limit_bytes=1024 * 1024),
        cost_estimate=pl.CostEstimate(flops=size, bytes_accessed=size, transcendentals=0),
        name="fetch",
    )(*[pltpu.with_memory_space_constraint(array, pltpu.HBM) for array in arrays], after)


def expert_kernel(part_ref, *refs, count, step, pieces):
    blocks, (gate_ref, up_ref, down_ref), rest = refs[:count], refs[count:count + 3], refs[count + 3:]
    out_refs, (rows_ref, act_ref, acc_ref) = rest[:-3], rest[-3:]
    hidden, model = gate_ref.shape
    size = blocks[0].shape[0]
    for j, block in enumerate(blocks):
        rows_ref[j * size:(j + 1) * size] = block[...]
    rows = rows_ref[...]
    for start, stop in steps_of(hidden, step):
        gate = lax.dot_general(gate_ref[start:stop], rows, TURNED, preferred_element_type=jnp.float32)
        up = lax.dot_general(up_ref[start:stop], rows, TURNED, preferred_element_type=jnp.float32)
        act = gate * jax.nn.sigmoid(1.702 * gate) * (up + 1.0)
        act_ref[:, start:stop] = act.T.astype(jnp.bfloat16)
    act = act_ref[...]
    for start, stop in steps_of(model, 4 * LANES):
        acc_ref[:, start:stop] = jnp.dot(act, down_ref[:, start:stop], preferred_element_type=jnp.float32)
    chunks = len(out_refs) // pieces
    width = out_refs[0].shape[1]
    for shift in range(pieces):
        for i in range(pieces):

            @pl.when(part_ref[0] == (i - shift) % pieces)
            def _():
                start = 0
                for out_ref in out_refs[shift * chunks:(shift + 1) * chunks]:
                    stop = start + out_ref.shape[0]
                    out_ref[...] = acc_ref[start:stop, i * width:(i + 1) * width].astype(out_ref.dtype)
                    start = stop


def expert(part, blocks, gate, up, down, pieces, sizes, step=4 * LANES):
    size, model = blocks[0].shape
    count = size * len(blocks)
    hidden = gate.shape[0]
    vm = pl.BlockSpec(memory_space=pltpu.VMEM)
    return pl.pallas_call(
        functools.partial(expert_kernel, count=len(blocks), step=step, pieces=pieces),
        out_shape=[jax.ShapeDtypeStruct((n * size, model // pieces), jnp.bfloat16) for _ in range(pieces) for n in sizes],
        in_specs=[pl.BlockSpec(memory_space=pltpu.SMEM)] + [vm] * (len(blocks) + 3),
        out_specs=[vm] * (pieces * len(sizes)),
        scratch_shapes=[
            pltpu.VMEM((count, model), jnp.bfloat16),
            pltpu.VMEM((count, hidden), jnp.bfloat16),
            pltpu.VMEM((count, model), jnp.float32),
        ],
        compiler_params=pltpu.CompilerParams(vmem_limit_bytes=20 * 1024 * 1024),
        cost_estimate=pl.CostEstimate(flops=6 * count * model * hidden, bytes_accessed=6 * model * hidden, transcendentals=0),
        name="expert",
    )(part.astype(jnp.int32).reshape(1), *blocks, gate, up, down)


def gather_kernel(*refs, count):
    total = refs[0][...].astype(jnp.float32)
    for ref in refs[1:count]:
        total = total + ref[...].astype(jnp.float32)
    total = total.astype(jnp.bfloat16)
    for j, out_ref in enumerate(refs[count:]):
        out_ref[...] = total[j * CAP:(j + 1) * CAP]


def gather_parts(parts):
    rows, width = parts[0].shape
    vm = pl.BlockSpec(memory_space=pltpu.VMEM)
    return pl.pallas_call(
        functools.partial(gather_kernel, count=len(parts)),
        out_shape=[jax.ShapeDtypeStruct((CAP, width), jnp.bfloat16)] * (rows // CAP),
        in_specs=[vm] * len(parts),
        out_specs=[vm] * (rows // CAP),
        compiler_params=pltpu.CompilerParams(vmem_limit_bytes=8 * 1024 * 1024),
        cost_estimate=pl.CostEstimate(flops=rows * width * len(parts), bytes_accessed=2 * rows * width, transcendentals=0),
        name="gather_parts",
    )(*parts)


def portions(total):
    cuts = [total * k // 16 for k in (0, 3, 7, 12, 16)]
    return [b - a for a, b in zip(cuts, cuts[1:])]


def pack_kernel(tokens_ref, parts_refs, gain_ref, select_ref, resid_ref, *out_refs):
    resid = tokens_ref[...].astype(jnp.float32)
    for part_ref in parts_refs:
        resid = resid + part_ref[...].astype(jnp.float32)
    scale = lax.rsqrt(jnp.mean(resid * resid, axis=-1, keepdims=True) + 1e-05)
    resid_ref[...] = resid
    normed = (resid * scale * gain_ref[...]).astype(jnp.bfloat16)
    for start, stop in steps_of(normed.shape[1], 4 * LANES):
        piece = jnp.dot(select_ref[...], normed[:, start:stop], preferred_element_type=jnp.float32)
        for j, out_ref in enumerate(out_refs):
            out_ref[:, start:stop] = piece[j * CAP:(j + 1) * CAP].astype(jnp.bfloat16)


def pack(tokens, parts, gain, select):
    count, model = tokens.shape
    vm = pl.BlockSpec(memory_space=pltpu.VMEM)
    slots = select.shape[0]

    def whole(*refs):
        tokens_ref, parts, rest = refs[0], refs[1:1 + number], refs[1 + number:]
        pack_kernel(tokens_ref, parts, *rest)

    number = len(parts)
    return pl.pallas_call(
        whole,
        out_shape=[jax.ShapeDtypeStruct((count, model), jnp.float32)]
        + [jax.ShapeDtypeStruct((CAP, model), jnp.bfloat16)] * (slots // CAP),
        in_specs=[vm] * (3 + number),
        out_specs=[vm] * (1 + slots // CAP),
        compiler_params=pltpu.CompilerParams(vmem_limit_bytes=16 * 1024 * 1024),
        cost_estimate=pl.CostEstimate(flops=2 * slots * count * model, bytes_accessed=2 * slots * model, transcendentals=0),
        name="pack",
    )(tokens, *parts, gain.reshape(1, model), select)


def project_kernel(x_ref, weight_hbm, out_ref, weight_ref, acc_ref, sems, *, step):
    cuts = steps_of(weight_hbm.shape[0], step)
    copies = [pltpu.make_async_copy(weight_hbm.at[start:stop], weight_ref.at[start:stop], sems.at[i]) for i, (start, stop) in enumerate(cuts)]
    for copy in copies:
        copy.start()
    for i, (start, stop) in enumerate(cuts):
        copies[i].wait()
        part = jnp.dot(x_ref[:, start:stop], weight_ref[start:stop], preferred_element_type=jnp.float32)
        if i == 0:
            acc_ref[...] = part
        else:
            acc_ref[...] += part
    out_ref[...] = acc_ref[...].astype(out_ref.dtype)


def project(x, weight, step=2 * LANES):
    tokens, model = x.shape
    width = weight.shape[1]
    vm = pl.BlockSpec(memory_space=pltpu.VMEM)
    return pl.pallas_call(
        functools.partial(project_kernel, step=step),
        out_shape=jax.ShapeDtypeStruct((tokens, width), jnp.bfloat16),
        in_specs=[vm, pl.BlockSpec(memory_space=pl.ANY)],
        out_specs=vm,
        scratch_shapes=[
            pltpu.VMEM((model, width), jnp.bfloat16),
            pltpu.VMEM((tokens, width), jnp.float32),
            pltpu.SemaphoreType.DMA((pl.cdiv(model, step),)),
        ],
        compiler_params=pltpu.CompilerParams(vmem_limit_bytes=56 * 1024 * 1024),
        cost_estimate=pl.CostEstimate(flops=2 * tokens * model * width, bytes_accessed=2 * model * width, transcendentals=0),
        name="project",
    )(x, weight)


def combine_kernel(spread_ref, resid_ref, *refs):
    parts_ref, out_ref = refs[-1], refs[-2]
    for j, ref in enumerate(refs[:-2]):
        parts_ref[j * CAP:(j + 1) * CAP] = ref[...]
    spread = spread_ref[...]
    parts = parts_ref[...]
    total = resid_ref[...]
    for _ in range(3):
        coarse = spread.astype(jnp.bfloat16)
        spread = spread - coarse.astype(jnp.float32)
        total = total + jnp.dot(coarse, parts, preferred_element_type=jnp.float32)
    out_ref[...] = total.astype(out_ref.dtype)


def combine(spread, parts, resid):
    vm = pl.BlockSpec(memory_space=pltpu.VMEM)
    count, width = resid.shape
    return pl.pallas_call(
        combine_kernel,
        out_shape=jax.ShapeDtypeStruct((count, width), jnp.bfloat16),
        in_specs=[vm] * (2 + len(parts)),
        out_specs=vm,
        scratch_shapes=[pltpu.VMEM((spread.shape[1], width), jnp.bfloat16)],
        compiler_params=pltpu.CompilerParams(vmem_limit_bytes=16 * 1024 * 1024),
        cost_estimate=pl.CostEstimate(flops=6 * count * width * spread.shape[1], bytes_accessed=2 * width * spread.shape[1], transcendentals=0),
        name="combine",
    )(spread, resid, *parts)


def shifted(block, axis, distance):
    size = lax.axis_size(axis)
    return lax.ppermute(block, axis, [(i, (i + distance) % size) for i in range(size)])


def body(
    stream,
    query_weight,
    cache_keys,
    cache_values,
    new_keys,
    new_values,
    out_weight,
    norm_gain,
    expert_ids,
    expert_weights,
    gate_weight,
    up_weight,
    down_weight,
):
    tokens = stream[0]
    count, model = tokens.shape
    cycles = lax.axis_size("ctx")
    heads = lax.axis_size("head")
    place = lax.axis_index("ctx")
    query = project(tokens, query_weight)

    def columns(x):
        return x[0].transpose(1, 2, 0)

    def padded(x):
        return jnp.pad(x, ((0, 0), (0, 0), (0, LANES - x.shape[2])))

    keys, values = columns(cache_keys), columns(cache_values)
    fresh_keys, fresh_values = padded(columns(new_keys)), padded(columns(new_values))
    packets = []
    block = query
    for d in range(cycles):
        following = shifted(block, "ctx", 1) if d < cycles - 1 else None
        packet = attend(place, (place - d) % cycles, block, keys, values, fresh_keys, fresh_values)
        kept = packet
        if d < cycles - 1:
            following, packet = lax.optimization_barrier((following, packet))
        packets.append(packet if d == 0 else shifted(packet, "ctx", -d))
        block = following
    group = query.shape[1] // LANES
    (mixing,) = fetch([out_weight.T], kept)
    projected = merge_project(packets, mixing, group)
    parts = [projected]
    for d in range(1, heads):
        parts.append(shifted(projected, "head", d))
    width = model // heads
    experts = lax.axis_size("seq") * lax.axis_size("ctx")
    slots = experts * CAP
    chosen = expert_ids[0].reshape(-1)
    onehot = (chosen[:, None] == lax.broadcasted_iota(jnp.int32, (1, experts), 1)).astype(jnp.int32)
    before = jnp.cumsum(onehot, axis=0) - onehot
    slot = jnp.sum(before * onehot, axis=1)
    own = (lax.axis_index("seq") * cycles + place).astype(jnp.int32)
    ahead = ((chosen - own) % experts * CAP + slot)[None, :] == lax.broadcasted_iota(jnp.int32, (slots, 1), 0)
    select = jnp.sum(ahead.astype(jnp.float32).reshape(slots, count, -1), axis=-1).astype(jnp.bfloat16)
    resid, *packed = pack(tokens, parts, norm_gain, select)
    resid_own = lax.dynamic_slice_in_dim(resid, lax.axis_index("head") * width, width, 1)
    arrived = [packed[0]]
    for j in range(1, experts):
        arrived.append(shifted(packed[j], ("seq", "ctx"), j))
    fetched = fetch([gate_weight[0].T, up_weight[0].T, down_weight[0]], packed[0])
    sizes = portions(experts)
    pieces = expert(lax.axis_index("head"), arrived[1:] + arrived[:1], *fetched, heads, sizes)
    crossed = []
    for k in range(len(sizes)):
        crossed.append([pieces[k]])
        for d in range(1, heads):
            crossed[k].append(shifted(pieces[d * len(sizes) + k], "head", d))
    returned, j = {}, 1
    for k in range(len(sizes)):
        gathered = gather_parts(crossed[k])
        for block in gathered:
            returned[j % experts] = shifted(block, ("seq", "ctx"), -j) if j < experts else block
            j += 1
    spread = jnp.where(ahead.T, expert_weights[0].reshape(-1)[:, None], 0.0)
    spread = jnp.sum(spread.reshape(count, -1, slots), axis=1)
    mixed = combine(spread, [returned[j] for j in range(experts)], resid_own)
    return mixed[None]


def solution(mesh):
    in_specs = (
        P("seq", "ctx", None),
        P(None, "head"),
        P("seq", "ctx", "head", None),
        P("seq", "ctx", "head", None),
        P("seq", "ctx", "head", None),
        P("seq", "ctx", "head", None),
        P("head", None),
        P(),
        P("seq", "ctx", None),
        P("seq", "ctx", None),
        P(("seq", "ctx"), None, "head"),
        P(("seq", "ctx"), None, "head"),
        P(("seq", "ctx"), "head", None),
    )
    out_specs = P("seq", "ctx", "head")
    return jax.shard_map(body, mesh=mesh, in_specs=in_specs, out_specs=out_specs, check_vma=False)
```
